32 devices in a mesh: tm: 8 (over z, core), state: 4 (over y, x).
Axes of the slice: x: 2, y: 2, z: 4, core: 2. Of those that a mesh axis runs over, the one named last changes fastest.
Arguments:
- increments: bfloat16 [8, 2048, 128], P('tm', 'state'), may hold values from -4 to 4
- propagators: bfloat16 [8, 2048, 2048], P('tm', 'state'), may hold values from -1.1 to 1.1
- inv_var: float32 [8, 2048], P('tm', 'state'), may hold values from 0.25 to 2
Outputs:
- forward_state: bfloat16 [8, 2048, 128], P('tm', 'state')
- adjoint: bfloat16 [8, 2048, 128], P('tm', 'state')
The draws below stay inside these ranges and needn't reach their ends.
All inputs are finite; a program needn't handle non-finite values.
Results may differ from the reference program's by a relative error of at most 0.03.
Values may be sent and summed in bfloat16 or wider, within the bound.
A program may use at most 64 MiB of HBM per device.

```python
import math
import jax
import jax.numpy as jnp
from jax import lax

SDIM = 2048
COLS = 128
WINDOWS = 8


def draw_propagators(key, part):
    first, second = jax.random.split(jax.random.fold_in(key, 11))
    diagonal = jax.random.uniform(first, (WINDOWS, SDIM), jnp.float32, 0.97, 1.0)
    remainder = jax.random.truncated_normal(second, -4.0, 4.0, (WINDOWS, SDIM, SDIM), jnp.float32) * (0.3 / math.sqrt(SDIM))
    identity = jnp.eye(SDIM, dtype=jnp.float32)
    return (remainder + diagonal[:, :, None] * identity[None]).astype(jnp.bfloat16)


def block_scale(own_key, extent, cuts, low, high):
    factor_of, own = 1.0, jax.random.fold_in(own_key, 6)
    for dim, parts in cuts:
        heights = jnp.exp(jax.random.uniform(jax.random.fold_in(own, dim), (parts,), jnp.float32, low / len(cuts), high / len(cuts)))
        factor_of = factor_of * jnp.repeat(heights, extent[dim] // parts).reshape([-1 if axis == dim else 1 for axis in range(len(extent))])
    return factor_of


def gaussian(stream_key, dims, width, most, cuts=(), kind=jnp.bfloat16):
    gain = block_scale(stream_key, dims, cuts, -0.22, 0.18) if cuts else 1.0
    drawn = jax.random.normal(stream_key, dims, jnp.float32) * width * gain
    return jnp.minimum(jnp.maximum(drawn, -most), most).astype(kind)


def setup_inputs(seed: int = 0) -> dict:
    streams_of = jax.random.split(jax.random.key(seed), 4)
    return {
        "increments": gaussian(streams_of[0], (WINDOWS, SDIM, COLS), 0.3, 4.0, ((0, 8), (1, 4))),
        "propagators": draw_propagators(jax.random.fold_in(streams_of[3], 71), 0),
        "inv_var": jnp.clip(jnp.exp(math.log(2.0) - 2.0794415 * jax.random.uniform(streams_of[2], (WINDOWS, SDIM), jnp.float32) ** block_scale(streams_of[2], (WINDOWS, SDIM), ((0, 8), (1, 4)), -0.2, 0.2)), 0.25, 2.0),
    }


def reference(increments, propagators, inv_var):
    def forward_step(previous, inputs):
        matrix, driving = inputs
        current = (jnp.dot(matrix, previous, preferred_element_type=jnp.float32) + driving.astype(jnp.float32)).astype(jnp.bfloat16)
        return current, current

    start = jnp.zeros(increments.shape[1:], jnp.bfloat16)
    finished, forward_state = lax.scan(forward_step, start, (propagators, increments))
    weighted = inv_var[:, :, None] * forward_state.astype(jnp.float32)

    def backward_step(carry, inputs):
        matrix, weight_now = inputs
        current = (weight_now + carry).astype(jnp.bfloat16)
        passed = lax.dot_general(matrix, current, (((0,), (0,)), ((), ())), preferred_element_type=jnp.float32)
        return passed, current

    blank = jnp.zeros(weighted.shape[1:], jnp.float32)
    leftover, adjoint = lax.scan(backward_step, blank, (propagators, weighted), reverse=True)
    return forward_state, adjoint
```

```python
import functools

import jax
import jax.numpy as jnp
from jax import lax
from jax.experimental import pallas as pl
from jax.experimental.pallas import tpu as pltpu
from jax.sharding import PartitionSpec as P

MESH = pl.DeviceIdType.MESH
CHUNK = 32


def partner(s, d, n):
    if n & (n - 1):
        return lax.rem(s + d, n)
    bit, out = 1, s
    while bit < n:
        if d & bit:
            out = out + bit - 2 * bit * lax.rem(s // bit, 2)
        bit *= 2
    return out


def kernel(T, n, C, inc_ref, p_hbm, w_ref, f_ref, a_ref, p, pt, x, r, q, p_sem, fs, fr, bs, br):
    t, s = lax.axis_index("tm"), lax.axis_index("state")
    rows, dim = p.shape
    parts = p_sem.shape[0]
    part = rows // parts

    def load(i):
        cut = pl.ds(i * part, part)
        return pltpu.make_async_copy(p_hbm.at[0, cut, :], p.at[cut, :], p_sem.at[i])

    for i in range(parts):
        load(i).start()

    def neighbours(fn):
        @pl.when(t > 0)
        def _():
            fn(t - 1)

        @pl.when(t < T - 1)
        def _():
            fn(t + 1)

    barrier = pltpu.get_barrier_semaphore()

    def greet(other):
        for j in range(n):
            pl.semaphore_signal(barrier, inc=1, device_id=(other, j), device_id_type=MESH)

    neighbours(greet)
    turned = inc_ref[0].T
    for c in range(C):
        f_ref[c] = turned[c * CHUNK:(c + 1) * CHUNK, :]
    middle = jnp.logical_and(t > 0, t < T - 1)

    @pl.when(middle)
    def _():
        pl.semaphore_wait(barrier, 2 * n)

    @pl.when(jnp.logical_not(middle))
    def _():
        pl.semaphore_wait(barrier, n)

    def forward_copy(c, d, index, to):
        return pltpu.make_async_remote_copy(
            src_ref=f_ref.at[c], dst_ref=x.at[c, index], send_sem=fs.at[c, d],
            recv_sem=fr.at[c, index], device_id=to, device_id_type=MESH)

    def backward_copy(c, d, index, to):
        return pltpu.make_async_remote_copy(
            src_ref=q.at[c, d], dst_ref=r.at[c, index], send_sem=bs.at[c, d],
            recv_sem=br.at[c, index], device_id=to, device_id_type=MESH)

    def forward_send(c):
        @pl.when(t < T - 1)
        def _():
            for d in reversed(range(n)):
                forward_copy(c, d, s, (t + 1, partner(s, d, n))).start()

    def backward(c, last):
        weighted = w_ref[...] * f_ref[c].astype(jnp.float32)
        if not last:
            for d in range(n):
                j = partner(s, d, n)
                backward_copy(c, d, j, (t, s)).wait_recv()
                weighted += r[c, j].astype(jnp.float32)
        current = weighted.astype(jnp.bfloat16)
        a_ref[c] = current

        @pl.when(t > 0)
        def _():
            for d in reversed(range(n)):
                j = partner(s, d, n)
                cut = pl.ds(pl.multiple_of(j * rows, rows), rows)
                term = jnp.dot(current, p[:, cut], preferred_element_type=jnp.float32)
                q[c, d] = term.astype(jnp.bfloat16)
                backward_copy(c, d, s, (t - 1, j)).start()

    @pl.when(t == 0)
    def _():
        @pl.loop(0, C)
        def _(c):
            forward_send(c)

        for i in range(parts):
            load(i).wait()

    @pl.when(t > 0)
    def _():
        for i in range(parts):
            load(i).wait()
        block = 128

        @pl.loop(0, dim // block)
        def _(i):
            cut = pl.ds(pl.multiple_of(i * block, block), block)
            pt[cut, :] = p[:, cut].T

        @pl.loop(0, C)
        def _(c):
            total = f_ref[c].astype(jnp.float32)
            for d in range(n):
                j = partner(s, d, n)
                forward_copy(c, d, j, (t, s)).wait_recv()
                cut = pl.ds(pl.multiple_of(j * rows, rows), rows)
                total += jnp.dot(x[c, j], pt[cut, :], preferred_element_type=jnp.float32)
            f_ref[c] = total.astype(jnp.bfloat16)
            forward_send(c)

            @pl.when(t == T - 1)
            def _():
                backward(c, True)

    @pl.when(t < T - 1)
    def _():
        @pl.loop(0, C)
        def _(c):
            backward(c, False)

    @pl.loop(0, C)
    def _(c):
        for d in range(n):
            @pl.when(t < T - 1)
            def _():
                forward_copy(c, d, s, (t, s)).wait_send()

            @pl.when(t > 0)
            def _():
                backward_copy(c, d, s, (t, s)).wait_send()


def solution(mesh):
    T, n = mesh.shape["tm"], mesh.shape["state"]

    def step(increments, propagators, inv_var):
        _, rows, cols = increments.shape
        dim = propagators.shape[2]
        C = cols // CHUNK
        out = jax.ShapeDtypeStruct((C, CHUNK, rows), jnp.bfloat16)
        vmem = pl.BlockSpec(memory_space=pltpu.VMEM)
        f, a = pl.pallas_call(
            functools.partial(kernel, T, n, C),
            out_shape=(out, out),
            in_specs=[vmem, pl.BlockSpec(memory_space=pl.ANY), vmem],
            out_specs=(vmem, vmem),
            scratch_shapes=[
                pltpu.VMEM((rows, dim), jnp.bfloat16),
                pltpu.VMEM((dim, rows), jnp.bfloat16),
                pltpu.VMEM((C, n, CHUNK, rows), jnp.bfloat16),
                pltpu.VMEM((C, n, CHUNK, rows), jnp.bfloat16),
                pltpu.VMEM((C, n, CHUNK, rows), jnp.bfloat16),
                pltpu.SemaphoreType.DMA((4,)),
                pltpu.SemaphoreType.DMA((C, n)),
                pltpu.SemaphoreType.DMA((C, n)),
                pltpu.SemaphoreType.DMA((C, n)),
                pltpu.SemaphoreType.DMA((C, n)),
            ],
            compiler_params=pltpu.CompilerParams(collective_id=0, has_side_effects=True),
        )(increments, propagators, inv_var)
        return (f.reshape(cols, rows).T[None], a.reshape(cols, rows).T[None])

    return jax.shard_map(
        step, mesh=mesh,
        in_specs=(P("tm", "state", None), P("tm", "state", None), P("tm", "state")),
        out_specs=(P("tm", "state", None), P("tm", "state", None)), check_vma=False)
```

```python
import functools

import jax
import jax.numpy as jnp
from jax import lax
from jax.experimental import pallas as pl
from jax.experimental.pallas import tpu as pltpu
from jax.sharding import PartitionSpec as P

MESH = pl.DeviceIdType.MESH
CHUNK = 16


def partner(s, d, n):
    if n & (n - 1):
        return lax.rem(s + d, n)
    bit, out = 1, s
    while bit < n:
        if d & bit:
            out = out + bit - 2 * bit * lax.rem(s // bit, 2)
        bit *= 2
    return out


def kernel(T, n, C, inc_hbm, p_hbm, w_hbm, f_hbm, a_hbm, inc_ref, w_ref, f_ref, a_ref, whole, p, pt, x, r, q,
           in_sem, out_sem, p_sem, fs, fr, bs, br):
    t, s = lax.axis_index("tm"), lax.axis_index("state")
    rows, dim = p.shape
    parts = p_sem.shape[0]
    part = rows // parts

    def load(i):
        cut = pl.ds(i * part, part)
        return pltpu.make_async_copy(p_hbm.at[0, cut, :], p.at[cut, :], p_sem.at[i])

    inc_load = pltpu.make_async_copy(inc_hbm.at[0], inc_ref, in_sem.at[0])
    w_load = pltpu.make_async_copy(w_hbm, w_ref, in_sem.at[1])
    inc_load.start()
    w_load.start()
    for i in range(parts):
        load(i).start()

    def neighbours(fn):
        @pl.when(t > 0)
        def _():
            fn(t - 1)

        @pl.when(t < T - 1)
        def _():
            fn(t + 1)

    barrier = pltpu.get_barrier_semaphore()

    def greet(other):
        for j in range(n):
            pl.semaphore_signal(barrier, inc=1, device_id=(other, j), device_id_type=MESH)

    neighbours(greet)
    inc_load.wait()
    turned = inc_ref[...].T
    for c in range(C):
        f_ref[c] = turned[c * CHUNK:(c + 1) * CHUNK, :]
    middle = jnp.logical_and(t > 0, t < T - 1)

    @pl.when(middle)
    def _():
        pl.semaphore_wait(barrier, 2 * n)

    @pl.when(jnp.logical_not(middle))
    def _():
        pl.semaphore_wait(barrier, n)

    def forward_copy(c, d, index, to):
        return pltpu.make_async_remote_copy(
            src_ref=f_ref.at[c], dst_ref=x.at[c, index], send_sem=fs.at[c, d],
            recv_sem=fr.at[c, index], device_id=to, device_id_type=MESH)

    def backward_copy(c, d, index, to):
        return pltpu.make_async_remote_copy(
            src_ref=q.at[c, d], dst_ref=r.at[c, index], send_sem=bs.at[c, d],
            recv_sem=br.at[c, index], device_id=to, device_id_type=MESH)

    def store(k, source, target):
        for c in range(C):
            joined = source[c] if c == 0 else jnp.concatenate([joined, source[c]], axis=0)
        whole[k] = joined.T
        return pltpu.make_async_copy(whole.at[k], target.at[0], out_sem.at[k])

    def forward_send(c):
        @pl.when(t < T - 1)
        def _():
            for d in reversed(range(n)):
                forward_copy(c, d, s, (t + 1, partner(s, d, n))).start()

    def backward(c, last):
        weighted = w_ref[...] * f_ref[c].astype(jnp.float32)
        if not last:
            for d in range(n):
                j = partner(s, d, n)
                backward_copy(c, d, j, (t, s)).wait_recv()
                weighted += r[c, j].astype(jnp.float32)
        current = weighted.astype(jnp.bfloat16)
        a_ref[c] = current

        @pl.when(t > 0)
        def _():
            for d in reversed(range(n)):
                j = partner(s, d, n)
                cut = pl.ds(pl.multiple_of(j * rows, rows), rows)
                term = jnp.dot(current, p[:, cut], preferred_element_type=jnp.float32)
                q[c, d] = term.astype(jnp.bfloat16)
                backward_copy(c, d, s, (t - 1, j)).start()

    w_load.wait()

    @pl.when(t == 0)
    def _():
        @pl.loop(0, C)
        def _(c):
            forward_send(c)

        for i in range(parts):
            load(i).wait()

    @pl.when(t > 0)
    def _():
        for i in range(parts):
            load(i).wait()
        block = 128

        @pl.loop(0, dim // block)
        def _(i):
            cut = pl.ds(pl.multiple_of(i * block, block), block)
            pt[cut, :] = p[:, cut].T

        @pl.loop(0, C)
        def _(c):
            total = f_ref[c].astype(jnp.float32)
            for d in range(n):
                j = partner(s, d, n)
                forward_copy(c, d, j, (t, s)).wait_recv()
                cut = pl.ds(pl.multiple_of(j * rows, rows), rows)
                total += jnp.dot(x[c, j], pt[cut, :], preferred_element_type=jnp.float32)
            f_ref[c] = total.astype(jnp.bfloat16)
            forward_send(c)

            @pl.when(t == T - 1)
            def _():
                backward(c, True)

    f_store = store(0, f_ref, f_hbm)
    f_store.start()

    @pl.when(t < T - 1)
    def _():
        @pl.loop(0, C)
        def _(c):
            backward(c, False)

    a_store = store(1, a_ref, a_hbm)
    a_store.start()

    @pl.loop(0, C)
    def _(c):
        for d in range(n):
            @pl.when(t < T - 1)
            def _():
                forward_copy(c, d, s, (t, s)).wait_send()

            @pl.when(t > 0)
            def _():
                backward_copy(c, d, s, (t, s)).wait_send()

    f_store.wait()
    a_store.wait()


def solution(mesh):
    T, n = mesh.shape["tm"], mesh.shape["state"]

    def step(increments, propagators, inv_var):
        _, rows, cols = increments.shape
        dim = propagators.shape[2]
        C = cols // CHUNK
        out = jax.ShapeDtypeStruct((1, rows, cols), jnp.bfloat16)
        hbm = pl.BlockSpec(memory_space=pl.ANY)
        return pl.pallas_call(
            functools.partial(kernel, T, n, C),
            out_shape=(out, out),
            in_specs=[hbm] * 3,
            out_specs=(hbm, hbm),
            scratch_shapes=[
                pltpu.VMEM((rows, cols), jnp.bfloat16),
                pltpu.VMEM((1, rows), jnp.float32),
                pltpu.VMEM((C, CHUNK, rows), jnp.bfloat16),
                pltpu.VMEM((C, CHUNK, rows), jnp.bfloat16),
                pltpu.VMEM((2, rows, cols), jnp.bfloat16),
                pltpu.VMEM((rows, dim), jnp.bfloat16),
                pltpu.VMEM((dim, rows), jnp.bfloat16),
                pltpu.VMEM((C, n, CHUNK, rows), jnp.bfloat16),
                pltpu.VMEM((C, n, CHUNK, rows), jnp.bfloat16),
                pltpu.VMEM((C, n, CHUNK, rows), jnp.bfloat16),
                pltpu.SemaphoreType.DMA((2,)),
                pltpu.SemaphoreType.DMA((2,)),
                pltpu.SemaphoreType.DMA((4,)),
                pltpu.SemaphoreType.DMA((C, n)),
                pltpu.SemaphoreType.DMA((C, n)),
                pltpu.SemaphoreType.DMA((C, n)),
                pltpu.SemaphoreType.DMA((C, n)),
            ],
            compiler_params=pltpu.CompilerParams(collective_id=0, has_side_effects=True),
        )(increments, propagators, inv_var)

    return jax.shard_map(
        step, mesh=mesh,
        in_specs=(P("tm", "state", None), P("tm", "state", None), P("tm", "state")),
        out_specs=(P("tm", "state", None), P("tm", "state", None)), check_vma=False)
```

```python
import functools

import jax
import jax.numpy as jnp
from jax import lax
from jax.experimental import pallas as pl
from jax.experimental.pallas import tpu as pltpu
from jax.sharding import PartitionSpec as P

MESH = pl.DeviceIdType.MESH
CHUNK = 16


def partner(s, d, n):
    if n & (n - 1):
        return lax.rem(s + d, n)
    bit, out = 1, s
    while bit < n:
        if d & bit:
            out = out + bit - 2 * bit * lax.rem(s // bit, 2)
        bit *= 2
    return out


def kernel(T, n, C, inc_hbm, p_hbm, w_hbm, f_hbm, a_hbm, inc_ref, w_ref, f_ref, a_ref, whole, p, pt, x, r, q,
           in_sem, out_sem, p_sem, fs, fr, bs, br):
    t, s = lax.axis_index("tm"), lax.axis_index("state")
    rows, dim = p.shape
    parts = p_sem.shape[0]
    part = rows // parts

    def load(i):
        cut = pl.ds(i * part, part)
        return pltpu.make_async_copy(p_hbm.at[0, cut, :], p.at[cut, :], p_sem.at[i])

    inc_load = pltpu.make_async_copy(inc_hbm.at[0], inc_ref, in_sem.at[0])
    w_load = pltpu.make_async_copy(w_hbm, w_ref, in_sem.at[1])
    inc_load.start()
    w_load.start()
    for i in range(parts):
        load(i).start()

    def neighbours(fn):
        @pl.when(t > 0)
        def _():
            fn(t - 1)

        @pl.when(t < T - 1)
        def _():
            fn(t + 1)

    barrier = pltpu.get_barrier_semaphore()

    def greet(other):
        for j in range(n):
            pl.semaphore_signal(barrier, inc=1, device_id=(other, j), device_id_type=MESH)

    neighbours(greet)
    inc_load.wait()
    turned = inc_ref[...].T
    for c in range(C):
        f_ref[c] = turned[c * CHUNK:(c + 1) * CHUNK, :]
    middle = jnp.logical_and(t > 0, t < T - 1)

    @pl.when(middle)
    def _():
        pl.semaphore_wait(barrier, 2 * n)

    @pl.when(jnp.logical_not(middle))
    def _():
        pl.semaphore_wait(barrier, n)

    def forward_copy(c, d, index, to):
        return pltpu.make_async_remote_copy(
            src_ref=f_ref.at[c], dst_ref=x.at[c, index], send_sem=fs.at[c, d],
            recv_sem=fr.at[c, index], device_id=to, device_id_type=MESH)

    def backward_copy(c, d, index, to):
        return pltpu.make_async_remote_copy(
            src_ref=q.at[c, d], dst_ref=r.at[c, index], send_sem=bs.at[c, d],
            recv_sem=br.at[c, index], device_id=to, device_id_type=MESH)

    def store(k, source, target):
        for c in range(C):
            joined = source[c] if c == 0 else jnp.concatenate([joined, source[c]], axis=0)
        whole[k] = joined.T
        return pltpu.make_async_copy(whole.at[k], target.at[0], out_sem.at[k])

    def forward_send(c):
        @pl.when(t < T - 1)
        def _():
            for d in reversed(range(n)):
                forward_copy(c, d, s, (t + 1, partner(s, d, n))).start()

    def stacked(blocks):
        return blocks[0] if len(blocks) == 1 else jnp.concatenate(blocks, axis=0)

    def forward(cs):
        total = stacked([f_ref[c] for c in cs]).astype(jnp.float32)
        for d in range(n):
            j = partner(s, d, n)
            for c in cs:
                forward_copy(c, d, j, (t, s)).wait_recv()
            cut = pl.ds(pl.multiple_of(j * rows, rows), rows)
            total += jnp.dot(stacked([x[c, j] for c in cs]), pt[cut, :], preferred_element_type=jnp.float32)
        current = total.astype(jnp.bfloat16)
        for k, c in enumerate(cs):
            f_ref[c] = current[k * CHUNK:(k + 1) * CHUNK, :]

    def backward(cs, last):
        weighted = w_ref[...] * stacked([f_ref[c] for c in cs]).astype(jnp.float32)
        if not last:
            for d in range(n):
                j = partner(s, d, n)
                for c in cs:
                    backward_copy(c, d, j, (t, s)).wait_recv()
                weighted += stacked([r[c, j] for c in cs]).astype(jnp.float32)
        current = weighted.astype(jnp.bfloat16)
        for k, c in enumerate(cs):
            a_ref[c] = current[k * CHUNK:(k + 1) * CHUNK, :]

        @pl.when(t > 0)
        def _():
            def term(d):
                cut = pl.ds(pl.multiple_of(partner(s, d, n) * rows, rows), rows)
                return jnp.dot(current, p[:, cut], preferred_element_type=jnp.float32).astype(jnp.bfloat16)

            def send(d, value):
                for k, c in enumerate(cs):
                    q[c, d] = value[k * CHUNK:(k + 1) * CHUNK, :]
                    backward_copy(c, d, s, (t - 1, partner(s, d, n))).start()

            ready = term(n - 1)
            for d in reversed(range(n - 1)):
                following = term(d)
                send(d + 1, ready)
                ready = following
            send(0, ready)

    def turn(cs):
        forward(cs)
        backward(cs, True)

    w_load.wait()

    @pl.when(t == 0)
    def _():
        @pl.loop(0, C)
        def _(c):
            forward_send(c)

        for i in range(parts):
            load(i).wait()

    @pl.when(t > 0)
    def _():
        for i in range(parts):
            load(i).wait()
        block = 128

        @pl.loop(0, dim // block)
        def _(i):
            cut = pl.ds(pl.multiple_of(i * block, block), block)
            pt[cut, :] = p[:, cut].T

        @pl.when(t < T - 1)
        def _():
            @pl.loop(0, C)
            def _(c):
                forward([c])
                forward_send(c)

        @pl.when(t == T - 1)
        def _():
            pairs = (C - 2) // 2
            turn([0])

            @pl.loop(0, pairs)
            def _(i):
                turn([1 + 2 * i, 2 + 2 * i])

            for c in range(1 + 2 * pairs, C):
                turn([c])

    f_store = store(0, f_ref, f_hbm)
    f_store.start()

    @pl.when(t < T - 1)
    def _():
        @pl.loop(0, C)
        def _(c):
            backward([c], False)

    a_store = store(1, a_ref, a_hbm)
    a_store.start()

    @pl.loop(0, C)
    def _(c):
        for d in range(n):
            @pl.when(t < T - 1)
            def _():
                forward_copy(c, d, s, (t, s)).wait_send()

            @pl.when(t > 0)
            def _():
                backward_copy(c, d, s, (t, s)).wait_send()

    f_store.wait()
    a_store.wait()


def hand_on(f_in, a_in, f_out, a_out, buffer, sems):
    pairs = ((f_in, f_out), (a_in, a_out))
    loads = [pltpu.make_async_copy(src, buffer.at[k], sems.at[k]) for k, (src, _) in enumerate(pairs)]
    stores = [pltpu.make_async_copy(buffer.at[k], dst, sems.at[2 + k]) for k, (_, dst) in enumerate(pairs)]
    for load in loads:
        load.start()
    for load, store in zip(loads, stores):
        load.wait()
        store.start()
    for store in stores:
        store.wait()


def solution(mesh):
    T, n = mesh.shape["tm"], mesh.shape["state"]

    def step(increments, propagators, inv_var):
        _, rows, cols = increments.shape
        dim = propagators.shape[2]
        C = cols // CHUNK
        out = jax.ShapeDtypeStruct((1, rows, cols), jnp.bfloat16)
        hbm = pl.BlockSpec(memory_space=pl.ANY)
        f, a = pl.pallas_call(
            functools.partial(kernel, T, n, C),
            out_shape=(out, out),
            in_specs=[hbm] * 3,
            out_specs=(hbm, hbm),
            scratch_shapes=[
                pltpu.VMEM((rows, cols), jnp.bfloat16),
                pltpu.VMEM((1, rows), jnp.float32),
                pltpu.VMEM((C, CHUNK, rows), jnp.bfloat16),
                pltpu.VMEM((C, CHUNK, rows), jnp.bfloat16),
                pltpu.VMEM((2, rows, cols), jnp.bfloat16),
                pltpu.VMEM((rows, dim), jnp.bfloat16),
                pltpu.VMEM((dim, rows), jnp.bfloat16),
                pltpu.VMEM((C, n, CHUNK, rows), jnp.bfloat16),
                pltpu.VMEM((C, n, CHUNK, rows), jnp.bfloat16),
                pltpu.VMEM((C, n, CHUNK, rows), jnp.bfloat16),
                pltpu.SemaphoreType.DMA((2,)),
                pltpu.SemaphoreType.DMA((2,)),
                pltpu.SemaphoreType.DMA((4,)),
                pltpu.SemaphoreType.DMA((C, n)),
                pltpu.SemaphoreType.DMA((C, n)),
                pltpu.SemaphoreType.DMA((C, n)),
                pltpu.SemaphoreType.DMA((C, n)),
            ],
            compiler_params=pltpu.CompilerParams(collective_id=0, has_side_effects=True),
        )(increments, propagators, inv_var)
        return pl.pallas_call(
            hand_on,
            out_shape=(out, out),
            in_specs=[hbm] * 2,
            out_specs=(hbm, hbm),
            scratch_shapes=[pltpu.VMEM((2, 1, rows, cols), jnp.bfloat16), pltpu.SemaphoreType.DMA((4,))],
        )(f, a)

    return jax.shard_map(
        step, mesh=mesh,
        in_specs=(P("tm", "state", None), P("tm", "state", None), P("tm", "state")),
        out_specs=(P("tm", "state", None), P("tm", "state", None)), check_vma=False)
```
